256 devices in a mesh: rel: 2 (over y_hi), row: 8 (over y_lo, x), col: 16 (over z, core).
Axes of the slice: x: 4, y: 4 (y_hi: 2, y_lo: 2; y = y_hi * 2 + y_lo), z: 8, core: 2. Of those that a mesh axis runs over, the one named last changes fastest.
Arguments:
- features: float32 [4, 128, 256, 128], P('rel', ('row', 'col')), may hold values from -6 to 6
- lap_tiles: bfloat16 [4, 8, 16, 16, 256, 256], P('rel', 'row', 'col'), may hold values from -0.046875 to 0.046875
- tile_rows: int32 [4, 8, 16, 16], P('rel', 'row', 'col'), may hold values from 0 to 15
- tile_cols: int32 [4, 8, 16, 16], P('rel', 'row', 'col'), may hold values from 0 to 7
- tile_count: int32 [4, 8, 16], P('rel', 'row', 'col'), may hold values from 2 to 16, as said below
- cheb_coefs: float32 [4, 5], P('rel'), may hold values from -1 to 1
- merging_weight: bfloat16 [512, 128], replicated, may hold values from -0.25 to 0.25
Outputs:
- merged_rows: float32 [128, 256, 128], P(('row', 'col'), 'rel')
The draws below stay inside these ranges and needn't reach their ends.
Inputs may be any that keep to these rules, and one draw needn't show every extreme that they name: Only the first tile_count slots of a device count; in every relation some device has 16 valid slots.
All inputs are finite; a program needn't handle non-finite values.
Results may differ from the reference program's by a relative error of at most 0.0063.
Values may be sent and summed in bfloat16 or wider, within the bound.
No kernel may reach another device: no remote copies, remote signals or barrier semaphores. Data moves between devices by JAX's collectives and lax.ppermute only.
A program may use at most 64 MiB of HBM per device.

```python
import jax
import jax.numpy as jnp
from jax import lax

D = 128
TILE = 256
ORDERS = 4
PB = 1
TPD = 16
RELS = 4
PIECES = 128
PIECE_ROWS = 256
BLOCKS = 128
N_ROW = 8
N_COL = 16


def draw_tile_count(key, part):
    shift_key, pick_key = jax.random.split(key)
    levels = jnp.array([TPD, TPD // 2, TPD // 4, TPD // 8], dtype=jnp.int32)
    shifts = jax.random.randint(shift_key, (RELS, N_ROW * N_COL), 0, 4)
    counts = levels[shifts]
    chosen = jax.random.randint(pick_key, (RELS, 1), 0, N_ROW * N_COL)
    counts = jnp.where(jnp.arange(N_ROW * N_COL, dtype=jnp.int32)[None, :] == chosen, TPD, counts)
    return counts.reshape(RELS, N_ROW, N_COL).astype(jnp.int32)


def plant(drawn, own_key, low, high):
    shape = drawn.shape
    index_at = [jax.random.randint(jax.random.fold_in(own_key, axis), (), 0, shape[axis]) for axis in range(len(shape))]
    drawn = drawn.at[tuple(index_at)].set(low)
    longest = shape.index(max(shape))
    index_at[longest] = (index_at[longest] + 1) % shape[longest]
    return drawn.at[tuple(index_at)].set(high)


def block_levels(key, extent, shards, low, high):
    loudness = 1.0
    for dim, shards_of in shards:
        heights = jax.random.uniform(jax.random.fold_in(jax.random.fold_in(key, 6), dim), (shards_of,), jnp.float32, low / len(shards), high / len(shards))
        loudness = loudness * jnp.repeat(jnp.exp(heights), extent[dim] // shards_of).reshape((-1,) + (1,) * (len(extent) - 1 - dim))
    return loudness


def normal_values(stream_key, extent, deviation, bound, cuts=(), kind=jnp.bfloat16):
    level = block_levels(stream_key, extent, cuts, -0.22, 0.18) if cuts else 1.0
    drawn = jax.random.normal(stream_key, extent, jnp.float32) * deviation * level
    return jnp.minimum(jnp.maximum(drawn, -bound), bound).astype(kind)


def setup_inputs(seed: int = 0) -> dict:
    key_list = jax.random.split(jax.random.key(seed), 8)
    return {
        "features": normal_values(key_list[0], (RELS, PIECES, PIECE_ROWS, D), 1.0, 6.0, ((0, 2), (1, 128)), jnp.float32),
        "lap_tiles": normal_values(key_list[1], (RELS, N_ROW, N_COL, TPD, TILE, TILE), (4 * TILE * TPD // PB) ** -0.5, 0.046875, ((0, 2), (1, 8), (2, 16))),
        "tile_rows": plant(jax.random.randint(key_list[2], (RELS, N_ROW, N_COL, TPD), 0, N_COL * PB), jax.random.fold_in(key_list[2], 1), 0, (N_COL * PB) - 1).astype(jnp.int32),
        "tile_cols": plant(jax.random.randint(key_list[3], (RELS, N_ROW, N_COL, TPD), 0, N_ROW * PB), jax.random.fold_in(key_list[3], 1), 0, (N_ROW * PB) - 1).astype(jnp.int32),
        "tile_count": draw_tile_count(jax.random.fold_in(key_list[7], 71), 0),
        "cheb_coefs": jnp.clip(jax.random.uniform(key_list[5], (RELS, ORDERS + 1), jnp.float32, -1.0, 1.0) * block_levels(key_list[5], (RELS, ORDERS + 1), ((0, 2),), -0.4, 0.0), -1.0, 1.0),
        "merging_weight": normal_values(key_list[6], (RELS * D, D), (RELS * D) ** -0.5, 0.25),
    }


def shard_product(lap_tiles, tile_rows, tile_cols, tile_count, operand):
    blocks = operand.astype(jnp.float32).reshape(BLOCKS, TILE, D)
    col_index = jnp.arange(N_COL, dtype=jnp.int32)[:, None]
    slot_index = jnp.arange(TPD, dtype=jnp.int32)[None, :]

    def one_shard(inputs):
        shard_tiles, shard_rows, shard_cols, shard_count = inputs
        piece_index = (shard_cols // PB) * N_COL + col_index
        global_block = (piece_index * PB + shard_cols % PB).astype(jnp.int32)
        sources = blocks[global_block]
        products = jnp.einsum("cpab,cpbd->cpad", shard_tiles.astype(jnp.float32), sources,
                              precision=lax.Precision.HIGHEST)
        live_mask = (slot_index < shard_count[:, None]).astype(jnp.float32)
        products = products * live_mask[:, :, None, None]
        return jax.ops.segment_sum(products.reshape(N_COL * TPD, TILE, D),
                                   shard_rows.reshape(-1).astype(jnp.int32),
                                   num_segments=N_COL * PB)

    result = lax.map(one_shard, (lap_tiles, tile_rows, tile_cols, tile_count))
    return result.reshape(BLOCKS * TILE, D)


def reference(features, lap_tiles, tile_rows, tile_cols, tile_count, cheb_coefs, merging_weight):
    embeddings = []
    for relation in range(RELS):
        current = features[relation].reshape(BLOCKS * TILE, D)
        earlier = current
        embedding = cheb_coefs[relation, 0] * current
        for degree in range(1, ORDERS + 1):
            applied = shard_product(lap_tiles[relation], tile_rows[relation], tile_cols[relation],
                                    tile_count[relation], current.astype(jnp.bfloat16))
            if degree == 1:
                following = applied
            else:
                following = 2.0 * applied - earlier
            earlier, current = current, following
            embedding = embedding + cheb_coefs[relation, degree] * current
        embeddings.append(embedding.astype(jnp.bfloat16))
    joined = jnp.concatenate(embeddings, axis=1)
    merged_rows = jnp.dot(joined, merging_weight, preferred_element_type=jnp.float32)
    return merged_rows.reshape(PIECES, PIECE_ROWS, D)
```

```python
import jax
import jax.numpy as jnp
from jax import lax
from jax.experimental import pallas as pl
from jax.experimental.pallas import tpu as pltpu
from jax.sharding import PartitionSpec as P

ORDERS = 4
X = 4
Y = 2
Z = 8
UNROLL = 8


def row_shift(x, dx, dy):
    pairs = [(j * X + i, ((j + dy) % Y) * X + (i + dx) % X) for j in range(Y) for i in range(X)]
    return lax.ppermute(x, "row", pairs)


def z_shift(x, s):
    pairs = [(z * 2 + c, ((z + s) % Z) * 2 + c) for z in range(Z) for c in range(2)]
    return lax.ppermute(x, "col", pairs)


def core_swap(x):
    return lax.ppermute(x, "col", [(z * 2 + c, z * 2 + 1 - c) for z in range(Z) for c in range(2)])


def product_kernel(table, source, first, second, sums):
    def clear(k, carry):
        sums[k] = jnp.zeros(sums.shape[1:], sums.dtype)
        return carry

    lax.fori_loop(0, Z, clear, 0)
    for half, tiles in enumerate((first, second)):

        def step(i, carry):
            for u in range(UNROLL):
                s = i * UNROLL + u
                operand = source[table[half, 2, s], table[half, 3, s]]
                product = jnp.dot(tiles[s], operand, preferred_element_type=jnp.float32)
                k, c = table[half, 0, s], table[half, 1, s]
                sums[k, c] = sums[k, c] + product
            return carry

        lax.fori_loop(0, (table[half, 4, 0] + UNROLL - 1) // UNROLL, step, 0)


def local_product(table, source, first, second):
    rows, width = source.shape[2:]
    vmem = pl.BlockSpec(memory_space=pltpu.VMEM)
    return pl.pallas_call(
        product_kernel,
        out_shape=jax.ShapeDtypeStruct((Z + 1, 2, rows, width), jnp.float32),
        in_specs=[pl.BlockSpec(memory_space=pltpu.SMEM), vmem, vmem, vmem],
        out_specs=vmem,
    )(table, source, first, second)


def gather(piece):
    return lax.all_to_all(jnp.broadcast_to(piece[None], (X * Y, *piece.shape)), "row", 0, 0, tiled=True)


def reduced(held):
    up = z_shift(held[4].astype(jnp.bfloat16), 1)
    down = z_shift(held[5].astype(jnp.bfloat16), -1)
    for k in (3, 2, 1):
        up = z_shift((up.astype(jnp.float32) + held[k]).astype(jnp.bfloat16), 1)
    for k in (6, 7):
        down = z_shift((down.astype(jnp.float32) + held[k]).astype(jnp.bfloat16), -1)
    return held[0] + up.astype(jnp.float32) + down.astype(jnp.float32)


def at(x, index, dim=0):
    return lax.dynamic_index_in_dim(x, index, dim, keepdims=False)


def local(features, lap_tiles, tile_rows, tile_cols, tile_count, cheb_coefs, merging_weight):
    rows, width = features.shape[2:]
    slots = lap_tiles.shape[3]
    rel = lax.axis_index("rel")
    col = lax.axis_index("col")
    core = col % 2
    tile_rows = tile_rows.reshape(2, slots)
    tile_cols = tile_cols.reshape(2, slots)
    count = tile_count.reshape(2, 1)
    live = jnp.arange(slots, dtype=jnp.int32)[None] < count
    target = (tile_rows // 2 - col // 2) % Z
    target = jnp.where(live, target, Z)
    side = jnp.broadcast_to(core, target.shape)
    table = jnp.stack([target, tile_rows % 2, tile_cols, side, jnp.broadcast_to(count, target.shape)], axis=1)
    table = jnp.stack([at(table, core), core_swap(at(table, 1 - core))])
    lap_tiles = lap_tiles.reshape(2, *lap_tiles.shape[3:])
    first = at(lap_tiles, core)
    second = core_swap(at(lap_tiles, 1 - core))
    features = features[:, 0]
    own = at(features, core)
    other = core_swap(at(features, 1 - core))
    current = jnp.where(core == 0, jnp.stack([own, other]), jnp.stack([other, own]))
    coefs = at(cheb_coefs, core)
    earlier = current
    embedding = coefs[0] * current
    for degree in range(1, ORDERS + 1):
        held = local_product(table, gather(current.astype(jnp.bfloat16)), first, second)
        applied = reduced(held)
        following = applied if degree == 1 else 2.0 * applied - earlier
        earlier, current = current, following
        embedding = embedding + coefs[degree] * following
    embedding = embedding.astype(jnp.bfloat16)
    own = at(embedding, core)
    other = core_swap(at(embedding, 1 - core))
    embedded = jnp.where(core == 0, jnp.stack([own, other]), jnp.stack([other, own]))
    half = rows // 2
    kept = lax.dynamic_slice_in_dim(embedded, rel * half, half, 1)
    given = lax.dynamic_slice_in_dim(embedded, (1 - rel) * half, half, 1)
    taken = lax.ppermute(given, "rel", [(0, 1), (1, 0)])
    weights = merging_weight.reshape(2, 2, width, width)
    merged = jnp.zeros((half, width), jnp.float32)
    for part, index in ((kept, rel), (taken, 1 - rel)):
        weight = at(weights, index)
        for r in range(2):
            merged = merged + jnp.dot(part[r], weight[r], preferred_element_type=jnp.float32)
    return merged[None]


def solution(mesh):
    placed = (
        P("rel", ("row", "col"), None, None),
        P("rel", "row", "col", None, None, None),
        P("rel", "row", "col", None),
        P("rel", "row", "col", None),
        P("rel", "row", "col"),
        P("rel", None),
        P(),
    )
    return jax.shard_map(
        local, mesh=mesh, in_specs=placed, out_specs=P(("row", "col"), "rel", None), check_vma=False
    )
```

```python
import jax
import jax.numpy as jnp
from jax import lax
from jax.experimental import pallas as pl
from jax.experimental.pallas import tpu as pltpu
from jax.sharding import PartitionSpec as P

ORDERS = 4
X = 4
Y = 2
Z = 8
UNROLL = 4
WHOLE = 4


def row_shift(x, dx, dy):
    pairs = [(j * X + i, ((j + dy) % Y) * X + (i + dx) % X) for j in range(Y) for i in range(X)]
    return lax.ppermute(x, "row", pairs)


def z_shift(x, s):
    pairs = [(z * 2 + c, ((z + s) % Z) * 2 + c) for z in range(Z) for c in range(2)]
    return lax.ppermute(x, "col", pairs)


def core_swap(x):
    return lax.ppermute(x, "col", [(z * 2 + c, z * 2 + 1 - c) for z in range(Z) for c in range(2)])


def at(x, index, dim=0):
    return lax.dynamic_index_in_dim(x, index, dim, keepdims=False)


def whole_kernel(table, source, *refs):
    sum_products(table, 5, source, *refs)


def pieces_kernel(table, own, beside, across, before, after, corner, *refs):
    refs, source = refs[:-1], refs[-1]
    for slot, piece in ((0, own), (2, across), (4, beside), (6, corner)):
        source[slot] = piece[...]
    for j in range(Y):
        source[j * X + 1] = before[j]
        source[j * X + 3] = after[j]
    sum_products(table, 2, source, *refs)


def sum_products(table, origin, source, first, second, sums, up, down, last):
    def clear(k, carry):
        sums[k] = jnp.zeros(sums.shape[1:], sums.dtype)
        return carry

    lax.fori_loop(0, Z, clear, 0)
    for half, tiles in enumerate((first, second)):

        def step(i, carry):
            for u in range(UNROLL):
                s = i * UNROLL + u
                operand = source[table[half, origin, s], table[half, 3, s]]
                product = jnp.dot(tiles[s], operand, preferred_element_type=jnp.float32)
                k, c = table[half, 0, s], table[half, 1, s]
                sums[k, c] = sums[k, c] + product
            return carry

        lax.fori_loop(0, (table[half, 4, 0] + UNROLL - 1) // UNROLL, step, 0)
    up[0] = sums[4].astype(up.dtype)
    up[1] = sums[2].astype(up.dtype)
    down[...] = sums[5].astype(down.dtype)
    last[...] = sums[7].astype(last.dtype)


def local_product(table, pieces, first, second):
    whole = len(pieces) == 1
    dims = pieces[0].shape[-3:]
    vmem = pl.BlockSpec(memory_space=pltpu.VMEM)
    return pl.pallas_call(
        whole_kernel if whole else pieces_kernel,
        out_shape=(
            pltpu.VMEM((Z + 1, *dims), jnp.float32),
            pltpu.VMEM((2, *dims), jnp.bfloat16),
            pltpu.VMEM(dims, jnp.bfloat16),
            pltpu.VMEM(dims, jnp.bfloat16),
        ),
        in_specs=[pl.BlockSpec(memory_space=pltpu.SMEM)] + [vmem] * (len(pieces) + 2),
        out_specs=(vmem, vmem, vmem, vmem),
        scratch_shapes=[] if whole else [pltpu.VMEM((X * Y, *dims), jnp.bfloat16)],
        compiler_params=pltpu.CompilerParams(vmem_limit_bytes=8 << 20),
    )(table, *(pltpu.with_memory_space_constraint(x, pltpu.VMEM) for x in (*pieces, first, second)))


def part_kernel(core, tiles, kept, given, sems):
    copies = [
        pltpu.make_async_copy(tiles.at[core[0]], kept, sems.at[0]),
        pltpu.make_async_copy(tiles.at[1 - core[0]], given, sems.at[1]),
    ]
    for copy in copies:
        copy.start()
    for copy in copies:
        copy.wait()


def parted(core, tiles):
    vmem = pl.BlockSpec(memory_space=pltpu.VMEM)
    part = pltpu.VMEM(tiles.shape[1:], tiles.dtype)
    return pl.pallas_call(
        part_kernel,
        out_shape=(part, part),
        in_specs=[pl.BlockSpec(memory_space=pltpu.SMEM), pl.BlockSpec(memory_space=pltpu.HBM)],
        out_specs=(vmem, vmem),
        scratch_shapes=[pltpu.SemaphoreType.DMA((2,))],
        compiler_params=pltpu.CompilerParams(vmem_limit_bytes=8 << 20),
    )(core[None], pltpu.with_memory_space_constraint(tiles, pltpu.HBM))


def gather(own):
    beside = row_shift(own, 0, 1)
    across = row_shift(own, 2, 0)
    both = jnp.stack([own, beside])
    before = row_shift(both, 1, 0)
    after = row_shift(both, -1, 0)
    corner = row_shift(across, 0, 1)
    return own, beside, across, before, after, corner


def gather_whole(own):
    return (lax.all_to_all(jnp.broadcast_to(own[None], (X * Y, *own.shape)), "row", 0, 0, tiled=True),)


def reduced(held, up, down, last):
    f32, bf16 = jnp.float32, jnp.bfloat16
    up = z_shift(up, 1)
    down = z_shift(down, -1)
    far = z_shift((held[3] + up[0].astype(f32)).astype(bf16), 3)
    low = z_shift((held[6] + down.astype(f32)).astype(bf16), -2)
    near = z_shift((held[1] + up[1].astype(f32)).astype(bf16), 1)
    last = z_shift(last, -1)
    return held[0] + far.astype(f32) + low.astype(f32) + near.astype(f32) + last.astype(f32)


def local(features, lap_tiles, tile_rows, tile_cols, tile_count, cheb_coefs, merging_weight):
    rows, width = features.shape[2:]
    slots = lap_tiles.shape[3]
    rel = lax.axis_index("rel")
    row = lax.axis_index("row")
    col = lax.axis_index("col")
    core = col % 2
    features = features[:, 0]
    own = at(features, core)
    given = at(features, 1 - core)
    other = core_swap(given)
    lap_tiles, other = lax.optimization_barrier((lap_tiles.reshape(2, *lap_tiles.shape[3:]), other))
    first, second = parted(core, lap_tiles)
    second = core_swap(second)
    current = jnp.where(core == 0, jnp.stack([own, other]), jnp.stack([other, own]))
    operand = current.astype(jnp.bfloat16)
    tile_rows, tile_cols, tile_count, operand = lax.optimization_barrier(
        (tile_rows, tile_cols, tile_count, operand)
    )
    tile_rows = tile_rows.reshape(2, slots)
    tile_cols = tile_cols.reshape(2, slots)
    count = tile_count.reshape(2, 1)
    live = jnp.arange(slots, dtype=jnp.int32)[None] < count
    target = (tile_rows // 2 - col // 2) % Z
    target = jnp.where(live, target, Z)
    origin = ((row // X - tile_cols // X) % Y) * X + (row - tile_cols) % X
    side = jnp.broadcast_to(core, target.shape)
    table = jnp.stack([target, tile_rows % 2, origin, side, jnp.broadcast_to(count, target.shape), tile_cols], axis=1)
    received = core_swap(at(table, 1 - core))
    table = jnp.stack([at(table, core), received])
    coefs = at(cheb_coefs, core)
    earlier = current
    embedding = coefs[0] * current
    for degree in range(1, ORDERS + 1):
        pieces = (gather_whole if degree == WHOLE else gather)(operand)
        held, up, down, last = local_product(table, pieces, first, second)
        held, embedding = lax.optimization_barrier((held, embedding))
        applied = reduced(held, up, down, last)
        following = applied if degree == 1 else 2.0 * applied - earlier
        earlier, current = current, following
        operand = current.astype(jnp.bfloat16)
        if degree < ORDERS:
            earlier, current, operand = lax.optimization_barrier((earlier, current, operand))
        embedding = embedding + coefs[degree] * current
    embedding = embedding.astype(jnp.bfloat16)
    own = at(embedding, core)
    other = core_swap(at(embedding, 1 - core))
    embedded = jnp.where(core == 0, jnp.stack([own, other]), jnp.stack([other, own]))
    half = rows // 2
    kept = lax.dynamic_slice_in_dim(embedded, rel * half, half, 1)
    given = lax.dynamic_slice_in_dim(embedded, (1 - rel) * half, half, 1)
    taken = lax.ppermute(given, "rel", [(0, 1), (1, 0)])
    weights = merging_weight.reshape(2, 2, width, width)
    merged = jnp.zeros((half, width), jnp.float32)
    for part, index in ((kept, rel), (taken, 1 - rel)):
        weight = at(weights, index)
        for r in range(2):
            merged = merged + jnp.dot(part[r], weight[r], preferred_element_type=jnp.float32)
    return merged[None]


def solution(mesh):
    placed = (
        P("rel", ("row", "col"), None, None),
        P("rel", "row", "col", None, None, None),
        P("rel", "row", "col", None),
        P("rel", "row", "col", None),
        P("rel", "row", "col"),
        P("rel", None),
        P(),
    )
    return jax.shard_map(
        local, mesh=mesh, in_specs=placed, out_specs=P(("row", "col"), "rel", None), check_vma=False
    )
```

```python
import jax
import jax.numpy as jnp
from jax import lax
from jax.experimental import pallas as pl
from jax.experimental.pallas import tpu as pltpu
from jax.sharding import PartitionSpec as P

ORDERS = 4
X = 4
Y = 2
Z = 8
UNROLL = 4
WHOLE = 4


def row_shift(x, dx, dy):
    pairs = [(j * X + i, ((j + dy) % Y) * X + (i + dx) % X) for j in range(Y) for i in range(X)]
    return lax.ppermute(x, "row", pairs)


def z_shift(x, s):
    pairs = [(z * 2 + c, ((z + s) % Z) * 2 + c) for z in range(Z) for c in range(2)]
    return lax.ppermute(x, "col", pairs)


def core_swap(x):
    return lax.ppermute(x, "col", [(z * 2 + c, z * 2 + 1 - c) for z in range(Z) for c in range(2)])


def at(x, index, dim=0):
    return lax.dynamic_index_in_dim(x, index, dim, keepdims=False)


def whole_kernel(table, source, *refs):
    sum_products(table, 5, source, *refs)


def pieces_kernel(table, own, beside, across, before, after, corner, *refs):
    refs, source = refs[:-1], refs[-1]
    for slot, piece in ((0, own), (2, across), (4, beside), (6, corner)):
        source[slot] = piece[...]
    for j in range(Y):
        source[j * X + 1] = before[j]
        source[j * X + 3] = after[j]
    sum_products(table, 2, source, *refs)


def sum_products(table, origin, source, first, second, sums, up, down, last):
    def clear(k, carry):
        sums[k] = jnp.zeros(sums.shape[1:], sums.dtype)
        return carry

    lax.fori_loop(0, Z, clear, 0)
    for half, tiles in enumerate((first, second)):

        def step(i, carry):
            for u in range(UNROLL):
                s = i * UNROLL + u
                operand = source[table[half, origin, s], table[half, 3, s]]
                product = jnp.dot(tiles[s], operand, preferred_element_type=jnp.float32)
                k, c = table[half, 0, s], table[half, 1, s]
                sums[k, c] = sums[k, c] + product
            return carry

        lax.fori_loop(0, (table[half, 4, 0] + UNROLL - 1) // UNROLL, step, 0)
    up[0] = sums[3].astype(up.dtype)
    up[1] = sums[1].astype(up.dtype)
    down[0] = sums[5].astype(down.dtype)
    down[1] = sums[7].astype(down.dtype)
    last[...] = sums[4].astype(last.dtype)


def local_product(table, pieces, first, second):
    whole = len(pieces) == 1
    dims = pieces[0].shape[-3:]
    vmem = pl.BlockSpec(memory_space=pltpu.VMEM)
    return pl.pallas_call(
        whole_kernel if whole else pieces_kernel,
        out_shape=(
            pltpu.VMEM((Z + 1, *dims), jnp.float32),
            pltpu.VMEM((2, *dims), jnp.bfloat16),
            pltpu.VMEM((2, *dims), jnp.bfloat16),
            pltpu.VMEM(dims, jnp.bfloat16),
        ),
        in_specs=[pl.BlockSpec(memory_space=pltpu.SMEM)] + [vmem] * (len(pieces) + 2),
        out_specs=(vmem, vmem, vmem, vmem),
        scratch_shapes=[] if whole else [pltpu.VMEM((X * Y, *dims), jnp.bfloat16)],
        compiler_params=pltpu.CompilerParams(vmem_limit_bytes=8 << 20),
    )(table, *(pltpu.with_memory_space_constraint(x, pltpu.VMEM) for x in (*pieces, first, second)))


def part_kernel(core, tiles, kept, given, sems):
    copies = [
        pltpu.make_async_copy(tiles.at[core[0]], kept, sems.at[0]),
        pltpu.make_async_copy(tiles.at[1 - core[0]], given, sems.at[1]),
    ]
    for copy in copies:
        copy.start()
    for copy in copies:
        copy.wait()


def parted(core, tiles):
    vmem = pl.BlockSpec(memory_space=pltpu.VMEM)
    part = pltpu.VMEM(tiles.shape[1:], tiles.dtype)
    return pl.pallas_call(
        part_kernel,
        out_shape=(part, part),
        in_specs=[pl.BlockSpec(memory_space=pltpu.SMEM), pl.BlockSpec(memory_space=pltpu.HBM)],
        out_specs=(vmem, vmem),
        scratch_shapes=[pltpu.SemaphoreType.DMA((2,))],
        compiler_params=pltpu.CompilerParams(vmem_limit_bytes=8 << 20),
    )(core[None], pltpu.with_memory_space_constraint(tiles, pltpu.HBM))


def gather(own):
    beside = row_shift(own, 0, 1)
    across = row_shift(own, 2, 0)
    both = jnp.stack([own, beside])
    before = row_shift(both, 1, 0)
    after = row_shift(both, -1, 0)
    corner = row_shift(across, 0, 1)
    return own, beside, across, before, after, corner


def gather_whole(own):
    return (lax.all_to_all(jnp.broadcast_to(own[None], (X * Y, *own.shape)), "row", 0, 0, tiled=True),)


def reduced(held, up, down, last):
    f32, bf16 = jnp.float32, jnp.bfloat16
    over = z_shift(last[0], 2)
    under = z_shift(last[1], -2)
    up = z_shift(up, 1)
    down = z_shift(down, -1)
    high = held[2] + up[0].astype(f32)
    high = z_shift(jnp.stack([high[0] + over.astype(f32), high[1]]).astype(bf16), 2)
    low = held[6] + down[0].astype(f32)
    low = z_shift(jnp.stack([low[0], low[1] + under.astype(f32)]).astype(bf16), -2)
    return held[0] + up[1].astype(f32) + down[1].astype(f32) + high.astype(f32) + low.astype(f32)


def local(features, lap_tiles, tile_rows, tile_cols, tile_count, cheb_coefs, merging_weight):
    rows, width = features.shape[2:]
    slots = lap_tiles.shape[3]
    rel = lax.axis_index("rel")
    row = lax.axis_index("row")
    col = lax.axis_index("col")
    core = col % 2
    features = features[:, 0]
    own = at(features, core)
    given = at(features, 1 - core)
    other = core_swap(given)
    lap_tiles, other = lax.optimization_barrier((lap_tiles.reshape(2, *lap_tiles.shape[3:]), other))
    first, second = parted(core, lap_tiles)
    second = core_swap(second)
    current = jnp.where(core == 0, jnp.stack([own, other]), jnp.stack([other, own]))
    operand = current.astype(jnp.bfloat16)
    tile_rows, tile_cols, tile_count, operand = lax.optimization_barrier(
        (tile_rows, tile_cols, tile_count, operand)
    )
    tile_rows = tile_rows.reshape(2, slots)
    tile_cols = tile_cols.reshape(2, slots)
    count = tile_count.reshape(2, 1)
    live = jnp.arange(slots, dtype=jnp.int32)[None] < count
    target = (tile_rows // 2 - col // 2) % Z
    target = jnp.where(live, target, Z)
    origin = ((row // X - tile_cols // X) % Y) * X + (row - tile_cols) % X
    side = jnp.broadcast_to(core, target.shape)
    table = jnp.stack([target, tile_rows % 2, origin, side, jnp.broadcast_to(count, target.shape), tile_cols], axis=1)
    received = core_swap(at(table, 1 - core))
    table = jnp.stack([at(table, core), received])
    coefs = at(cheb_coefs, core)
    earlier = current
    embedding = coefs[0] * current
    for degree in range(1, ORDERS + 1):
        pieces = (gather_whole if degree == WHOLE else gather)(operand)
        held, up, down, last = local_product(table, pieces, first, second)
        held, embedding = lax.optimization_barrier((held, embedding))
        applied = reduced(held, up, down, last)
        following = applied if degree == 1 else 2.0 * applied - earlier
        earlier, current = current, following
        operand = current.astype(jnp.bfloat16)
        if degree < ORDERS:
            earlier, current, operand = lax.optimization_barrier((earlier, current, operand))
        embedding = embedding + coefs[degree] * current
    embedding = embedding.astype(jnp.bfloat16)
    own = at(embedding, core)
    other = core_swap(at(embedding, 1 - core))
    embedded = jnp.where(core == 0, jnp.stack([own, other]), jnp.stack([other, own]))
    half = rows // 2
    kept = lax.dynamic_slice_in_dim(embedded, rel * half, half, 1)
    given = lax.dynamic_slice_in_dim(embedded, (1 - rel) * half, half, 1)
    taken = lax.ppermute(given, "rel", [(0, 1), (1, 0)])
    weights = merging_weight.reshape(2, 2, width, width)
    merged = jnp.zeros((half, width), jnp.float32)
    for part, index in ((kept, rel), (taken, 1 - rel)):
        weight = at(weights, index)
        for r in range(2):
            merged = merged + jnp.dot(part[r], weight[r], preferred_element_type=jnp.float32)
    return merged[None]


def solution(mesh):
    placed = (
        P("rel", ("row", "col"), None, None),
        P("rel", "row", "col", None, None, None),
        P("rel", "row", "col", None),
        P("rel", "row", "col", None),
        P("rel", "row", "col"),
        P("rel", None),
        P(),
    )
    return jax.shard_map(
        local, mesh=mesh, in_specs=placed, out_specs=P(("row", "col"), "rel", None), check_vma=False
    )
```

```python
import jax
import jax.numpy as jnp
from jax import lax
from jax.experimental import pallas as pl
from jax.experimental.pallas import tpu as pltpu
from jax.sharding import PartitionSpec as P

ORDERS = 4
X = 4
Y = 2
Z = 8
UNROLL = 8
WHOLE = 4


def row_shift(x, dx, dy):
    pairs = [(j * X + i, ((j + dy) % Y) * X + (i + dx) % X) for j in range(Y) for i in range(X)]
    return lax.ppermute(x, "row", pairs)


def z_shift(x, s):
    pairs = [(z * 2 + c, ((z + s) % Z) * 2 + c) for z in range(Z) for c in range(2)]
    return lax.ppermute(x, "col", pairs)


def core_swap(x):
    return lax.ppermute(x, "col", [(z * 2 + c, z * 2 + 1 - c) for z in range(Z) for c in range(2)])


def at(x, index, dim=0):
    return lax.dynamic_index_in_dim(x, index, dim, keepdims=False)


def whole_kernel(table, source, *refs):
    sum_products(table, 5, source, *refs)


def pieces_kernel(table, own, beside, across, before, after, corner, *refs):
    refs, source = refs[:-1], refs[-1]
    for slot, piece in ((0, own), (2, across), (4, beside), (6, corner)):
        source[slot] = piece[...]
    for j in range(Y):
        source[j * X + 1] = before[j]
        source[j * X + 3] = after[j]
    sum_products(table, 2, source, *refs)


def sum_products(table, origin, source, first, second, sums, up, down, last):
    def clear(k, carry):
        sums[k] = jnp.zeros(sums.shape[1:], sums.dtype)
        return carry

    lax.fori_loop(0, Z, clear, 0)
    for half, tiles in enumerate((first, second)):

        def step(i, carry):
            for u in range(UNROLL):
                s = i * UNROLL + u
                operand = source[table[half, origin, s], table[half, 3, s]]
                product = jnp.dot(tiles[s], operand, preferred_element_type=jnp.float32)
                k, c = table[half, 0, s], table[half, 1, s]
                sums[k, c] = sums[k, c] + product
            return carry

        lax.fori_loop(0, (table[half, 4, 0] + UNROLL - 1) // UNROLL, step, 0)
    up[0] = sums[3].astype(up.dtype)
    up[1] = sums[1].astype(up.dtype)
    down[0] = sums[5].astype(down.dtype)
    down[1] = sums[7].astype(down.dtype)
    last[...] = sums[4].astype(last.dtype)


def local_product(table, pieces, first, second):
    whole = len(pieces) == 1
    dims = pieces[0].shape[-3:]
    vmem = pl.BlockSpec(memory_space=pltpu.VMEM)
    return pl.pallas_call(
        whole_kernel if whole else pieces_kernel,
        out_shape=(
            pltpu.VMEM((Z + 1, *dims), jnp.float32),
            pltpu.VMEM((2, *dims), jnp.bfloat16),
            pltpu.VMEM((2, *dims), jnp.bfloat16),
            pltpu.VMEM(dims, jnp.bfloat16),
        ),
        in_specs=[pl.BlockSpec(memory_space=pltpu.SMEM)] + [vmem] * (len(pieces) + 2),
        out_specs=(vmem, vmem, vmem, vmem),
        scratch_shapes=[] if whole else [pltpu.VMEM((X * Y, *dims), jnp.bfloat16)],
        compiler_params=pltpu.CompilerParams(vmem_limit_bytes=8 << 20),
    )(table, *(pltpu.with_memory_space_constraint(x, pltpu.VMEM) for x in (*pieces, first, second)))


def part_kernel(core, tiles, kept, given, sems):
    copies = [
        pltpu.make_async_copy(tiles.at[core[0]], kept, sems.at[0]),
        pltpu.make_async_copy(tiles.at[1 - core[0]], given, sems.at[1]),
    ]
    for copy in copies:
        copy.start()
    for copy in copies:
        copy.wait()


def parted(core, tiles):
    vmem = pl.BlockSpec(memory_space=pltpu.VMEM)
    part = pltpu.VMEM(tiles.shape[1:], tiles.dtype)
    return pl.pallas_call(
        part_kernel,
        out_shape=(part, part),
        in_specs=[pl.BlockSpec(memory_space=pltpu.SMEM), pl.BlockSpec(memory_space=pltpu.HBM)],
        out_specs=(vmem, vmem),
        scratch_shapes=[pltpu.SemaphoreType.DMA((2,))],
        compiler_params=pltpu.CompilerParams(vmem_limit_bytes=8 << 20),
    )(core[None], pltpu.with_memory_space_constraint(tiles, pltpu.HBM))


def gather(own):
    beside = row_shift(own, 0, 1)
    across = row_shift(own, 2, 0)
    both = jnp.stack([own, beside])
    before = row_shift(both, 1, 0)
    after = row_shift(both, -1, 0)
    corner = row_shift(across, 0, 1)
    return own, beside, across, before, after, corner


def gather_whole(own):
    return (lax.all_to_all(jnp.broadcast_to(own[None], (X * Y, *own.shape)), "row", 0, 0, tiled=True),)


def reduced(held, up, down, last):
    f32, bf16 = jnp.float32, jnp.bfloat16
    over = z_shift(last[0], 2)
    under = z_shift(last[1], -2)
    up = z_shift(up, 1)
    down = z_shift(down, -1)
    high = held[2] + up[0].astype(f32)
    high = z_shift(jnp.stack([high[0] + over.astype(f32), high[1]]).astype(bf16), 2)
    low = held[6] + down[0].astype(f32)
    low = z_shift(jnp.stack([low[0], low[1] + under.astype(f32)]).astype(bf16), -2)
    return held[0] + up[1].astype(f32) + down[1].astype(f32) + high.astype(f32) + low.astype(f32)


def local(features, lap_tiles, tile_rows, tile_cols, tile_count, cheb_coefs, merging_weight):
    rows, width = features.shape[2:]
    slots = lap_tiles.shape[3]
    rel = lax.axis_index("rel")
    row = lax.axis_index("row")
    col = lax.axis_index("col")
    core = col % 2
    features = features[:, 0]
    own = at(features, core)
    given = at(features, 1 - core)
    other = core_swap(given)
    lap_tiles, other = lax.optimization_barrier((lap_tiles.reshape(2, *lap_tiles.shape[3:]), other))
    first, second = parted(core, lap_tiles)
    second = core_swap(second)
    current = jnp.where(core == 0, jnp.stack([own, other]), jnp.stack([other, own]))
    operand = current.astype(jnp.bfloat16)
    tile_rows, tile_cols, tile_count, operand = lax.optimization_barrier(
        (tile_rows, tile_cols, tile_count, operand)
    )
    tile_rows = tile_rows.reshape(2, slots)
    tile_cols = tile_cols.reshape(2, slots)
    count = tile_count.reshape(2, 1)
    live = jnp.arange(slots, dtype=jnp.int32)[None] < count
    target = (tile_rows // 2 - col // 2) % Z
    target = jnp.where(live, target, Z)
    origin = ((row // X - tile_cols // X) % Y) * X + (row - tile_cols) % X
    side = jnp.broadcast_to(core, target.shape)
    table = jnp.stack([target, tile_rows % 2, origin, side, jnp.broadcast_to(count, target.shape), tile_cols], axis=1)
    received = core_swap(at(table, 1 - core))
    table = jnp.stack([at(table, core), received])
    coefs = at(cheb_coefs, core)
    earlier = current
    embedding = coefs[0] * current
    for degree in range(1, ORDERS + 1):
        pieces = (gather_whole if degree == WHOLE else gather)(operand)
        held, up, down, last = local_product(table, pieces, first, second)
        held, embedding = lax.optimization_barrier((held, embedding))
        applied = reduced(held, up, down, last)
        following = applied if degree == 1 else 2.0 * applied - earlier
        earlier, current = current, following
        operand = current.astype(jnp.bfloat16)
        if degree < ORDERS:
            earlier, current, operand = lax.optimization_barrier((earlier, current, operand))
        embedding = embedding + coefs[degree] * current
    embedding = embedding.astype(jnp.bfloat16)
    own = at(embedding, core)
    other = core_swap(at(embedding, 1 - core))
    embedded = jnp.where(core == 0, jnp.stack([own, other]), jnp.stack([other, own]))
    half = rows // 2
    kept = lax.dynamic_slice_in_dim(embedded, rel * half, half, 1)
    given = lax.dynamic_slice_in_dim(embedded, (1 - rel) * half, half, 1)
    taken = lax.ppermute(given, "rel", [(0, 1), (1, 0)])
    weights = merging_weight.reshape(2, 2, width, width)
    merged = jnp.zeros((half, width), jnp.float32)
    for part, index in ((kept, rel), (taken, 1 - rel)):
        weight = at(weights, index)
        for r in range(2):
            merged = merged + jnp.dot(part[r], weight[r], preferred_element_type=jnp.float32)
    return merged[None]


def solution(mesh):
    placed = (
        P("rel", ("row", "col"), None, None),
        P("rel", "row", "col", None, None, None),
        P("rel", "row", "col", None),
        P("rel", "row", "col", None),
        P("rel", "row", "col"),
        P("rel", None),
        P(),
    )
    return jax.shard_map(
        local, mesh=mesh, in_specs=placed, out_specs=P(("row", "col"), "rel", None), check_vma=False
    )
```

```python
import jax
import jax.numpy as jnp
from jax import lax
from jax.experimental import pallas as pl
from jax.experimental.pallas import tpu as pltpu
from jax.sharding import PartitionSpec as P

ORDERS = 4
X = 4
Y = 2
Z = 8
UNROLL = 8
WHOLE = 4


def row_shift(x, dx, dy):
    pairs = [(j * X + i, ((j + dy) % Y) * X + (i + dx) % X) for j in range(Y) for i in range(X)]
    return lax.ppermute(x, "row", pairs)


def z_shift(x, s):
    pairs = [(z * 2 + c, ((z + s) % Z) * 2 + c) for z in range(Z) for c in range(2)]
    return lax.ppermute(x, "col", pairs)


def core_swap(x):
    return lax.ppermute(x, "col", [(z * 2 + c, z * 2 + 1 - c) for z in range(Z) for c in range(2)])


def at(x, index, dim=0):
    return lax.dynamic_index_in_dim(x, index, dim, keepdims=False)


def whole_kernel(table, source, *refs):
    sum_products(table, 5, source, *refs)


def pieces_kernel(table, own, beside, across, before, after, corner, *refs):
    refs, source = refs[:-1], refs[-1]
    for slot, piece in ((0, own), (2, across), (4, beside), (6, corner)):
        source[slot] = piece[...]
    for j in range(Y):
        source[j * X + 1] = before[j]
        source[j * X + 3] = after[j]
    sum_products(table, 2, source, *refs)


def sum_products(table, origin, source, first, second, sums, up, down, last):
    def clear(k, carry):
        sums[k] = jnp.zeros(sums.shape[1:], sums.dtype)
        return carry

    lax.fori_loop(0, Z, clear, 0)
    for half, tiles in enumerate((first, second)):

        def step(i, carry):
            for u in range(UNROLL):
                s = i * UNROLL + u
                operand = source[table[half, origin, s], table[half, 3, s]]
                product = jnp.dot(tiles[s], operand, preferred_element_type=jnp.float32)
                k, c = table[half, 0, s], table[half, 1, s]
                sums[k, c] = sums[k, c] + product
            return carry

        lax.fori_loop(0, (table[half, 4, 0] + UNROLL - 1) // UNROLL, step, 0)
    up[0] = sums[3].astype(up.dtype)
    up[1] = sums[1].astype(up.dtype)
    down[0] = sums[5].astype(down.dtype)
    down[1] = sums[7].astype(down.dtype)
    last[...] = sums[4].astype(last.dtype)


def local_product(table, pieces, first, second):
    whole = len(pieces) == 1
    dims = pieces[0].shape[-3:]
    vmem = pl.BlockSpec(memory_space=pltpu.VMEM)
    return pl.pallas_call(
        whole_kernel if whole else pieces_kernel,
        out_shape=(
            pltpu.VMEM((Z + 1, *dims), jnp.float32),
            pltpu.VMEM((2, *dims), jnp.bfloat16),
            pltpu.VMEM((2, *dims), jnp.bfloat16),
            pltpu.VMEM(dims, jnp.bfloat16),
        ),
        in_specs=[pl.BlockSpec(memory_space=pltpu.SMEM)] + [vmem] * (len(pieces) + 2),
        out_specs=(vmem, vmem, vmem, vmem),
        scratch_shapes=[] if whole else [pltpu.VMEM((X * Y, *dims), jnp.bfloat16)],
        compiler_params=pltpu.CompilerParams(vmem_limit_bytes=8 << 20),
    )(table, *(pltpu.with_memory_space_constraint(x, pltpu.VMEM) for x in (*pieces, first, second)))


def part_kernel(core, tiles, kept, given, sems):
    copies = [
        pltpu.make_async_copy(tiles.at[core[0]], kept, sems.at[0]),
        pltpu.make_async_copy(tiles.at[1 - core[0]], given, sems.at[1]),
    ]
    for copy in copies:
        copy.start()
    for copy in copies:
        copy.wait()


def parted(core, tiles):
    vmem = pl.BlockSpec(memory_space=pltpu.VMEM)
    part = pltpu.VMEM(tiles.shape[1:], tiles.dtype)
    return pl.pallas_call(
        part_kernel,
        out_shape=(part, part),
        in_specs=[pl.BlockSpec(memory_space=pltpu.SMEM), pl.BlockSpec(memory_space=pltpu.HBM)],
        out_specs=(vmem, vmem),
        scratch_shapes=[pltpu.SemaphoreType.DMA((2,))],
        compiler_params=pltpu.CompilerParams(vmem_limit_bytes=8 << 20),
    )(core[None], pltpu.with_memory_space_constraint(tiles, pltpu.HBM))


def gather(own):
    beside = row_shift(own, 0, 1)
    across = row_shift(own, 2, 0)
    both = jnp.stack([own, beside])
    before = row_shift(both, 1, 0)
    after = row_shift(both, -1, 0)
    corner = row_shift(across, 0, 1)
    return own, beside, across, before, after, corner


def gather_whole(own):
    return (lax.all_to_all(jnp.broadcast_to(own[None], (X * Y, *own.shape)), "row", 0, 0, tiled=True),)


def reduced(held, up, down, last):
    f32, bf16 = jnp.float32, jnp.bfloat16
    over = z_shift(last[0], 2)
    under = z_shift(last[1], -2)
    up = z_shift(up, 1)
    down = z_shift(down, -1)
    high = held[2] + up[0].astype(f32)
    high = z_shift(jnp.stack([high[0] + over.astype(f32), high[1]]).astype(bf16), 2)
    low = held[6] + down[0].astype(f32)
    low = z_shift(jnp.stack([low[0], low[1] + under.astype(f32)]).astype(bf16), -2)
    return held[0] + up[1].astype(f32) + down[1].astype(f32) + high.astype(f32) + low.astype(f32)


def local(features, lap_tiles, tile_rows, tile_cols, tile_count, cheb_coefs, merging_weight):
    rows, width = features.shape[2:]
    slots = lap_tiles.shape[3]
    rel = lax.axis_index("rel")
    row = lax.axis_index("row")
    col = lax.axis_index("col")
    core = col % 2
    features = features[:, 0]
    own = at(features, core)
    given = at(features, 1 - core)
    other = core_swap(given)
    lap_tiles, other = lax.optimization_barrier((lap_tiles.reshape(2, *lap_tiles.shape[3:]), other))
    first, second = parted(core, lap_tiles)
    second = core_swap(second)
    current = jnp.where(core == 0, jnp.stack([own, other]), jnp.stack([other, own]))
    operand = current.astype(jnp.bfloat16)
    tile_rows, tile_cols, tile_count, operand = lax.optimization_barrier(
        (tile_rows, tile_cols, tile_count, operand)
    )
    tile_rows = tile_rows.reshape(2, slots)
    tile_cols = tile_cols.reshape(2, slots)
    count = tile_count.reshape(2, 1)
    live = jnp.arange(slots, dtype=jnp.int32)[None] < count
    target = (tile_rows // 2 - col // 2) % Z
    target = jnp.where(live, target, Z)
    origin = ((row // X - tile_cols // X) % Y) * X + (row - tile_cols) % X
    side = jnp.broadcast_to(core, target.shape)
    table = jnp.stack([target, tile_rows % 2, origin, side, jnp.broadcast_to(count, target.shape), tile_cols], axis=1)
    received = core_swap(at(table, 1 - core))
    table = jnp.stack([at(table, core), received])
    coefs = at(cheb_coefs, core)
    earlier = current
    embedding = coefs[0] * current
    for degree in range(1, ORDERS + 1):
        pieces = (gather_whole if degree == WHOLE else gather)(operand)
        held, up, down, last = local_product(table, pieces, first, second)
        applied = reduced(held, up, down, last)
        following = applied if degree == 1 else 2.0 * applied - earlier
        earlier, current = current, following
        operand = current.astype(jnp.bfloat16)
        if degree < ORDERS:
            earlier, current, operand = lax.optimization_barrier((earlier, current, operand))
        embedding = embedding + coefs[degree] * current
    embedding = embedding.astype(jnp.bfloat16)
    own = at(embedding, core)
    other = core_swap(at(embedding, 1 - core))
    embedded = jnp.where(core == 0, jnp.stack([own, other]), jnp.stack([other, own]))
    half = rows // 2
    kept = lax.dynamic_slice_in_dim(embedded, rel * half, half, 1)
    given = lax.dynamic_slice_in_dim(embedded, (1 - rel) * half, half, 1)
    taken = lax.ppermute(given, "rel", [(0, 1), (1, 0)])
    weights = merging_weight.reshape(2, 2, width, width)
    merged = jnp.zeros((half, width), jnp.float32)
    for part, index in ((kept, rel), (taken, 1 - rel)):
        weight = at(weights, index)
        for r in range(2):
            merged = merged + jnp.dot(part[r], weight[r], preferred_element_type=jnp.float32)
    return merged[None]


def solution(mesh):
    placed = (
        P("rel", ("row", "col"), None, None),
        P("rel", "row", "col", None, None, None),
        P("rel", "row", "col", None),
        P("rel", "row", "col", None),
        P("rel", "row", "col"),
        P("rel", None),
        P(),
    )
    return jax.shard_map(
        local, mesh=mesh, in_specs=placed, out_specs=P(("row", "col"), "rel", None), check_vma=False
    )
```
